32 devices in a mesh: section: 2 (over x), dp: 16 (over z, y, core).
Axes of the slice: x: 2, y: 2, z: 4, core: 2. Of those that a mesh axis runs over, the one named last changes fastest.
Arguments:
- features: bfloat16 [1, 2, 2048, 4096], P(None, 'section', 'dp'), parts along dimension 2, may hold values from -6 to 6
- in_proj: bfloat16 [2, 4096, 512], P('section'), may hold values from -0.09375 to 0.09375
- mix_proj: bfloat16 [2, 2, 256, 256], P('section'), may hold values from -0.375 to 0.375
- out_proj: bfloat16 [2, 512, 4096], P('section'), may hold values from -0.375 to 0.375
- gate_proj: bfloat16 [2, 2, 4096], P('section'), may hold values from -0.09375 to 0.09375
- cross_bias: float32 [2, 4096], P('section'), may hold values from -3 to 3
Outputs:
- crossed: bfloat16 [1, 2, 2048, 4096], P(None, 'section', 'dp'), parts along dimension 2
The draws below stay inside these ranges and needn't reach their ends.
There are 16 independent parts, one for each index of `dp`. The reference program is written for one: setup_inputs(seed, part) draws one part's arguments, and reference() takes and returns one part's arrays. A program takes and returns all parts, laid end to end along the dimension named above; an argument that names none is the same for every part. Nothing has to cross between parts.
All inputs are finite; a program needn't handle non-finite values.
Results may differ from the reference program's by a relative error of at most 0.015.
Values may be sent and summed in bfloat16 or wider, within the bound.
A program may use at most 64 MiB of HBM per device.

```python
import jax
import jax.numpy as jnp
from jax import lax

D = 4096
RANK = 256
EXPERTS = 2
ROWS = 128
MB_DEV = 1
LAYERS = 2
N_SECTION = 2


def shard_levels(own_key, shape, split, low, high):
    level = 1.0
    for dim, parts in split:
        steps = jax.random.uniform(jax.random.fold_in(jax.random.fold_in(own_key, 6), dim), (parts,), jnp.float32, low / len(split), high / len(split))
        level = level * jnp.repeat(jnp.exp(steps), shape[dim] // parts).reshape((-1,) + (1,) * (len(shape) - 1 - dim))
    return level


def centred(rng, extent, spread, reach, shards=(), kind=jnp.bfloat16):
    entries = spread * jax.random.normal(rng, extent, jnp.float32)
    if shards:
        entries = entries * shard_levels(rng, extent, shards, -0.22, 0.18)
    return jnp.clip(entries, -reach, reach).astype(kind)


def setup_inputs(seed: int = 0, part: int = 0) -> dict:
    arg_keys = jax.random.split(jax.random.key(seed), 7)
    part_splits = jax.random.split(jax.random.fold_in(arg_keys[6], part), 7)
    return {
        "features": centred(part_splits[0], (MB_DEV, N_SECTION, ROWS, D), 1.0, 6.0, ((1, 2),)),
        "in_proj": centred(arg_keys[1], (LAYERS, D, EXPERTS * RANK), D ** -0.5, 0.09375, ((0, 2),)),
        "mix_proj": centred(arg_keys[2], (LAYERS, EXPERTS, RANK, RANK), RANK ** -0.5, 0.375, ((0, 2),)),
        "out_proj": centred(arg_keys[3], (LAYERS, EXPERTS * RANK, D), RANK ** -0.5, 0.375, ((0, 2),)),
        "gate_proj": centred(arg_keys[4], (LAYERS, EXPERTS, D), D ** -0.5, 0.09375, ((0, 2),)),
        "cross_bias": centred(arg_keys[5], (LAYERS, D), 0.5, 3.0, ((0, 2),), jnp.float32),
    }


def cross_layer(current, anchor, v_mat, c_mat, u_mat, gate_mat, shift_row):
    row_count = current.shape[0]
    expert_count = c_mat.shape[0]
    rank_size = c_mat.shape[1]
    projected = jnp.dot(current, v_mat, preferred_element_type=jnp.float32)
    inner_first = jnp.tanh(projected).astype(jnp.bfloat16).reshape(row_count, expert_count, rank_size)
    inner_second = jnp.einsum("rek,ekj->rej", inner_first.astype(jnp.float32), c_mat.astype(jnp.float32))
    logits = lax.dot_general(current, gate_mat, (((1,), (1,)), ((), ())), preferred_element_type=jnp.float32)
    gate_values = 1.0 / jnp.sum(jnp.exp(logits[:, None, :] - logits[:, :, None]), axis=2)
    blended = (gate_values[:, :, None] * jnp.tanh(inner_second)).astype(jnp.bfloat16)
    blended = blended.reshape(row_count, expert_count * rank_size)
    crossed = jnp.dot(blended, u_mat, preferred_element_type=jnp.float32)
    updated = current.astype(jnp.float32) + anchor.astype(jnp.float32) * (crossed + shift_row)
    return updated.astype(jnp.bfloat16)


def reference(features, in_proj, mix_proj, out_proj, gate_proj, cross_bias):
    anchor = features.reshape(-1, features.shape[-1])
    current = anchor
    for level in range(LAYERS):
        current = cross_layer(current, anchor, in_proj[level], mix_proj[level], out_proj[level], gate_proj[level], cross_bias[level])
    return current.reshape(features.shape)
```

```python
import jax

import jax.numpy as jnp
from jax import lax
from jax.experimental import pallas as pl
from jax.experimental.pallas import tpu as pltpu
from jax.sharding import PartitionSpec as P

CHUNKS = 8


def relay_kernel(
    x_hbm, v_hbm, c_hbm, u_hbm, g_hbm, b_hbm, o_hbm,
    xb, vb, cb, ub, gb, bb, in1, in2, out1, out2, ob, proj, lg, bl,
    lx, lv, lu, lw, s1, r1, s2, r2, so,
):
    chunks, rows, width = xb.shape
    experts, rank, _ = cb.shape
    me = lax.axis_index("section")
    peer = 1 - me

    def columns(c):
        return pl.ds(pl.multiple_of(c * width, width), width)

    def load_x(c):
        return pltpu.make_async_copy(x_hbm.at[:, columns(c)], xb.at[c], lx.at[c])

    def load_v(c):
        return pltpu.make_async_copy(v_hbm.at[columns(c)], vb.at[c], lv.at[c])

    def load_u(c):
        return pltpu.make_async_copy(u_hbm.at[:, columns(c)], ub.at[c], lu.at[c])

    load_c = pltpu.make_async_copy(c_hbm, cb, lw.at[0])
    load_g = pltpu.make_async_copy(g_hbm, gb, lw.at[1])
    load_b = pltpu.make_async_copy(b_hbm, bb, lw.at[2])

    def put(src, dst, send, recv, c):
        return pltpu.make_async_remote_copy(
            src_ref=src, dst_ref=dst.at[c], send_sem=send.at[c], recv_sem=recv.at[c],
            device_id={"section": peer}, device_id_type=pl.DeviceIdType.MESH,
        )

    def put_out(c):
        return pltpu.make_async_copy(ob.at[c], o_hbm.at[:, columns(c)], so.at[c])

    def each(body):
        def step(c, carry):
            body(c)
            return carry
        lax.fori_loop(0, chunks, step, 0)

    barrier = pltpu.get_barrier_semaphore()
    pl.semaphore_signal(
        barrier, inc=1, device_id={"section": peer}, device_id_type=pl.DeviceIdType.MESH
    )
    load_g.start()
    for c in range(chunks):
        load_x(c).start()
        load_v(c).start()
    load_c.start()
    load_b.start()
    for c in range(chunks):
        load_u(c).start()
    pl.semaphore_wait(barrier, 1)

    def project(source, arrive):
        proj[...] = jnp.zeros_like(proj)
        lg[...] = jnp.zeros_like(lg)

        def body(c):
            arrive(c)
            part = source[c]
            proj[...] += jnp.dot(part, vb[c], preferred_element_type=jnp.float32)
            lg[...] += lax.dot_general(
                part, gb[:, columns(c)], (((1,), (1,)), ((), ())),
                preferred_element_type=jnp.float32,
            )
        each(body)

    def mix():
        logits = lg[...]
        for e in range(experts):
            first = jnp.tanh(proj[:, e * rank:(e + 1) * rank]).astype(jnp.bfloat16)
            second = jnp.dot(first, cb[e], preferred_element_type=jnp.float32)
            total = jnp.sum(jnp.exp(logits - logits[:, e:e + 1]), axis=1, keepdims=True)
            gate = 1.0 / total
            bl[:, e * rank:(e + 1) * rank] = (gate * jnp.tanh(second)).astype(jnp.bfloat16)

    def crossed(c):
        return (
            jnp.dot(bl[...], ub[c], preferred_element_type=jnp.float32) + bb[:, columns(c)]
        )

    @pl.when(me == 0)
    def _():
        load_g.wait()

        def loaded(c):
            load_x(c).wait()
            load_v(c).wait()

        project(xb, loaded)
        load_c.wait()
        load_b.wait()
        mix()

        def own(c):
            load_u(c).wait()
            base = xb[c].astype(jnp.float32)
            out1[c] = (base + base * crossed(c)).astype(jnp.bfloat16)
            put(out1.at[c], in1, s1, r1, c).start()
        each(own)
        project(in1, lambda c: put(out1.at[c], in1, s1, r1, c).wait_recv())
        mix()

        def other(c):
            base = in1[c].astype(jnp.float32)
            out2[c] = (base + base * crossed(c)).astype(jnp.bfloat16)
            put(out2.at[c], in2, s2, r2, c).start()
        each(other)

        def finish(c):
            put(out2.at[c], in2, s2, r2, c).wait_recv()
            ob[c] = (
                out1[c].astype(jnp.float32)
                + xb[c].astype(jnp.float32) * in2[c].astype(jnp.float32)
            ).astype(jnp.bfloat16)
            put_out(c).start()
        each(finish)

        def drain(c):
            put(out1.at[c], in1, s1, r1, c).wait_send()
            put(out2.at[c], in2, s2, r2, c).wait_send()
            put_out(c).wait()
        each(drain)

    @pl.when(me == 1)
    def _():
        def send_x(c):
            return put(x_hbm.at[:, columns(c)], in1, s1, r1, c)

        each(lambda c: send_x(c).start())
        load_g.wait()
        load_c.wait()
        load_b.wait()

        def ready(c):
            load_x(c).wait()
            load_v(c).wait()
            load_u(c).wait()
        each(ready)
        project(in1, lambda c: send_x(c).wait_recv())
        mix()

        def back(c):
            out1[c] = crossed(c).astype(jnp.bfloat16)
            put(out1.at[c], in2, s2, r2, c).start()
        each(back)
        project(in2, lambda c: put(out1.at[c], in2, s2, r2, c).wait_recv())
        mix()

        def finish(c):
            ob[c] = (
                in2[c].astype(jnp.float32) + xb[c].astype(jnp.float32) * crossed(c)
            ).astype(jnp.bfloat16)
            put_out(c).start()
        each(finish)

        def drain(c):
            send_x(c).wait_send()
            put(out1.at[c], in2, s2, r2, c).wait_send()
            put_out(c).wait()
        each(drain)


def pair_device(features, in_proj, mix_proj, out_proj, gate_proj, cross_bias):
    rows, depth = features.shape[2:]
    experts, rank = mix_proj.shape[1:3]
    inner = experts * rank
    width = depth // CHUNKS
    kind = jnp.bfloat16
    block = pltpu.VMEM((CHUNKS, rows, width), kind)
    sems = pltpu.SemaphoreType.DMA((CHUNKS,))
    anywhere = pl.BlockSpec(memory_space=pl.ANY)
    out = pl.pallas_call(
        relay_kernel,
        out_shape=jax.ShapeDtypeStruct((rows, depth), kind),
        in_specs=[anywhere] * 6,
        out_specs=anywhere,
        scratch_shapes=[
            block,
            pltpu.VMEM((CHUNKS, width, inner), kind),
            pltpu.VMEM((experts, rank, rank), kind),
            pltpu.VMEM((CHUNKS, inner, width), kind),
            pltpu.VMEM((experts, depth), kind),
            pltpu.VMEM((1, depth), jnp.float32),
            block, block, block, block, block,
            pltpu.VMEM((rows, inner), jnp.float32),
            pltpu.VMEM((rows, experts), jnp.float32),
            pltpu.VMEM((rows, inner), kind),
            sems, sems, sems, pltpu.SemaphoreType.DMA((3,)),
            sems, sems, sems, sems, sems,
        ],
        compiler_params=pltpu.CompilerParams(
            collective_id=0, has_side_effects=True, vmem_limit_bytes=60 * 1024 * 1024
        ),
    )(features[0, 0], in_proj[0], mix_proj[0], out_proj[0], gate_proj[0], cross_bias)
    return out.reshape(features.shape)


def from_behind(block, axis, distance):
    devices = range(lax.axis_size(axis))
    route = [(i - distance, i) for i in devices if i - distance in devices]
    return lax.ppermute(block, axis, route)


def cross_layer(current, anchor, v_mat, c_mat, u_mat, gate_mat, shift_row):
    row_count = current.shape[0]
    expert_count = c_mat.shape[0]
    rank_size = c_mat.shape[1]
    projected = jnp.dot(current, v_mat, preferred_element_type=jnp.float32)
    inner_first = (
        jnp.tanh(projected).astype(jnp.bfloat16).reshape(row_count, expert_count, rank_size)
    )
    inner_second = jnp.einsum(
        "rek,ekj->rej", inner_first, c_mat, preferred_element_type=jnp.float32
    )
    logits = lax.dot_general(
        current, gate_mat, (((1,), (1,)), ((), ())), preferred_element_type=jnp.float32
    )
    gate_values = 1.0 / jnp.sum(jnp.exp(logits[:, None, :] - logits[:, :, None]), axis=2)
    blended = (gate_values[:, :, None] * jnp.tanh(inner_second)).astype(jnp.bfloat16)
    blended = blended.reshape(row_count, expert_count * rank_size)
    crossed = jnp.dot(blended, u_mat, preferred_element_type=jnp.float32)
    updated = current.astype(jnp.float32) + anchor.astype(jnp.float32) * (crossed + shift_row)
    return updated.astype(jnp.bfloat16)


def per_device(features, in_proj, mix_proj, out_proj, gate_proj, cross_bias):
    section_count = lax.axis_size("section")
    position = lax.axis_index("section")
    pieces = 1
    local_micro = features.shape[0]
    row_count = features.shape[2]
    feature_count = features.shape[3]
    piece_rows = row_count // pieces
    everyone = lax.all_gather(features, "section", axis=1, tiled=True)
    all_units = everyone.reshape(local_micro * section_count * pieces, piece_rows, feature_count)
    unit_count = all_units.shape[0]
    step_count = unit_count + section_count - 1
    v_mat = in_proj[0]
    c_mat = mix_proj[0]
    u_mat = out_proj[0]
    gate_mat = gate_proj[0]
    shift_row = cross_bias[0]

    def apply_layer(current, anchor):
        return cross_layer(current, anchor, v_mat, c_mat, u_mat, gate_mat, shift_row)

    def keep_input(current, anchor):
        return current

    def advance(carried, moment):
        incoming, outgoing, collected = carried
        unit_here = moment - position
        active = (unit_here >= 0) & (unit_here < unit_count)
        anchor = lax.dynamic_index_in_dim(
            all_units, jnp.clip(unit_here, 0, unit_count - 1), 0, keepdims=False
        )
        current = jnp.where(position == 0, anchor, incoming)
        result = lax.cond(active, apply_layer, keep_input, current, anchor)
        outgoing = jnp.where(position == section_count - 1, result, outgoing)
        held_unit = moment + position - 2 * section_count + 2
        arrived = (
            (held_unit >= 0)
            & (held_unit < unit_count)
            & (held_unit // pieces % section_count == position)
        )
        held_safe = jnp.clip(held_unit, 0, unit_count - 1)
        slot_index = held_safe // pieces // section_count * pieces + held_safe % pieces
        previous = lax.dynamic_index_in_dim(collected, slot_index, 0, keepdims=False)
        collected = lax.dynamic_update_index_in_dim(
            collected, jnp.where(arrived, outgoing, previous), slot_index, 0
        )
        return (result, outgoing, collected)

    def forward_step(carried, moment):
        result, outgoing, collected = advance(carried, moment)
        incoming = from_behind(result, "section", 1)
        return ((incoming, outgoing, collected), None)

    def cycle_step(carried, moment):
        moved, _ = forward_step(carried, moment)
        incoming, outgoing, collected = moved
        outgoing = from_behind(outgoing, "section", -1)
        return ((incoming, outgoing, collected), None)

    blank = jnp.zeros((piece_rows, feature_count), jnp.bfloat16)
    holding = jnp.zeros((local_micro * pieces, piece_rows, feature_count), jnp.bfloat16)
    carried, _ = lax.scan(
        forward_step, (blank, blank, holding), jnp.arange(0, section_count - 1, dtype=jnp.int32)
    )
    carried, _ = lax.scan(
        cycle_step, carried, jnp.arange(section_count - 1, step_count - 1, dtype=jnp.int32)
    )
    _, _, collected = advance(carried, jnp.int32(step_count - 1))
    return collected.reshape(local_micro, 1, row_count, feature_count)


def solution(mesh):
    placed = (
        P(None, "section", "dp", None),
        P("section", None, None),
        P("section", None, None, None),
        P("section", None, None),
        P("section", None, None),
        P("section", None),
    )
    sections = mesh.shape["section"]

    def choose(features, *weights):
        whole = sections == 2 and features.shape[0] == 1 and features.shape[3] % 1024 == 0
        return (pair_device if whole else per_device)(features, *weights)

    return jax.shard_map(
        choose,
        mesh=mesh,
        in_specs=placed,
        out_specs=P(None, "section", "dp", None),
        check_vma=False,
    )
```

```python
import jax
import jax.numpy as jnp
from jax import lax
from jax.experimental import pallas as pl
from jax.experimental.pallas import tpu as pltpu
from jax.sharding import PartitionSpec as P

GROUP = 4
MESH = pl.DeviceIdType.MESH


def relay_kernel(
    x_hbm, v_hbm, c_hbm, u_hbm, g_hbm, b_hbm, o_hbm,
    xb, vb, cb, ub, gb, bb, in1, out1, ob, gu, b2, proj, lg, bl, sent, got,
    lx, lv, lu, lw, s1, r1, so, sx, rg, s_up, s_down, s_side, s_core, s3, r3,
):
    chunks, rows, width = xb.shape
    experts, rank, _ = cb.shape
    layers = chunks // GROUP
    me = lax.axis_index("section")
    peer = 1 - me
    mine = lax.axis_index("dp")
    level = mine // GROUP
    core = mine % 2
    side = mine + 2 - 4 * (mine // 2 % 2)
    twin = mine + 1 - 2 * core

    def columns(c):
        return pl.ds(pl.multiple_of(c * width, width), width)

    def load_x(c):
        return pltpu.make_async_copy(x_hbm.at[:, columns(c)], xb.at[c], lx.at[c])

    def load_v(c):
        return pltpu.make_async_copy(v_hbm.at[columns(c)], vb.at[c], lv.at[c])

    def load_u(c):
        return pltpu.make_async_copy(u_hbm.at[:, columns(c)], ub.at[c], lu.at[c])

    load_c = pltpu.make_async_copy(c_hbm, cb, lw.at[0])
    load_g = pltpu.make_async_copy(g_hbm, gb, lw.at[1])
    load_b = pltpu.make_async_copy(b_hbm, bb, lw.at[2])

    def cross_over(src, dst, send, recv):
        return pltpu.make_async_remote_copy(
            src_ref=src, dst_ref=dst, send_sem=send, recv_sem=recv,
            device_id={"section": peer}, device_id_type=MESH,
        )

    def put(src, c):
        return cross_over(src, in1.at[c], s1.at[c], r1.at[c])

    def put_out(c):
        return pltpu.make_async_copy(ob.at[c], o_hbm.at[:, columns(c)], so.at[c])

    share_over = cross_over(u_hbm.at[:, columns(mine)], gu.at[mine], sx.at[0], rg.at[mine])
    bias_over = cross_over(b_hbm, b2, s3.at[0], r3.at[0])
    blend_over = cross_over(sent, got, s3.at[1], r3.at[1])

    def hand(share, target, send):
        return pltpu.make_async_remote_copy(
            src_ref=gu.at[share], dst_ref=gu.at[share], send_sem=send.at[share],
            recv_sem=rg.at[share], device_id={"dp": target}, device_id_type=MESH,
        )

    def await_share(share):
        hand(share, side, s_side).wait_recv()

    def pass_on(copy, finish):
        if finish:
            copy.wait_send()
        else:
            copy.start()

    def along(share, go_up, go_down, finish):
        if go_up:
            @pl.when(level < layers - 1)
            def _():
                pass_on(hand(share, mine + GROUP, s_up), finish)
        if go_down:
            @pl.when(level > 0)
            def _():
                pass_on(hand(share, mine - GROUP, s_down), finish)
        pass_on(hand(share, side, s_side), finish)
        pass_on(hand(share, twin, s_core), finish)

    def line_event(d, finish=False):
        def act(share, go_up, go_down):
            if not finish:
                await_share(share)
            along(share, go_up, go_down, finish)
        if d == 0:
            act(mine, True, True)
            return
        pl.when(level >= d)(lambda: act(mine - GROUP * d, True, False))
        pl.when(level + d < layers)(lambda: act(mine + GROUP * d, False, True))

    def side_event(d, finish=False):
        def act(share):
            if not finish:
                await_share(share)
            pass_on(hand(share, twin, s_core), finish)
        if d == 0:
            act(side)
            return
        pl.when(level >= d)(lambda: act(side - GROUP * d))
        pl.when(level + d < layers)(lambda: act(side + GROUP * d))

    def each(body, start=0, stop=chunks):
        def step(c, carry):
            body(c)
            return carry
        lax.fori_loop(start, stop, step, 0)

    barrier = pltpu.get_barrier_semaphore()
    pl.semaphore_signal(barrier, inc=1, device_id={"section": peer}, device_id_type=MESH)
    pl.semaphore_signal(barrier, inc=1, device_id={"dp": side}, device_id_type=MESH)
    pl.semaphore_signal(barrier, inc=1, device_id={"dp": twin}, device_id_type=MESH)

    @pl.when(level < layers - 1)
    def _():
        pl.semaphore_signal(barrier, inc=1, device_id={"dp": mine + GROUP}, device_id_type=MESH)

    @pl.when(level > 0)
    def _():
        pl.semaphore_signal(barrier, inc=1, device_id={"dp": mine - GROUP}, device_id_type=MESH)

    load_g.start()

    def load_first(c):
        load_x(c).start()
        load_v(c).start()
    each(load_first)
    load_c.start()
    load_b.start()
    each(lambda c: load_u(c).start())
    inside = (level > 0) & (level < layers - 1)

    @pl.when(inside)
    def _():
        pl.semaphore_wait(barrier, 5)

    @pl.when(jnp.logical_not(inside))
    def _():
        pl.semaphore_wait(barrier, 4 if layers > 1 else 3)

    share_over.start()
    bias_over.start()

    def clear():
        proj[...] = jnp.zeros_like(proj)
        lg[...] = jnp.zeros_like(lg)

    def gather_in(part, c):
        proj[...] += jnp.dot(part, vb[c], preferred_element_type=jnp.float32)
        lg[...] += lax.dot_general(
            part, gb[:, columns(c)], (((1,), (1,)), ((), ())),
            preferred_element_type=jnp.float32,
        )

    def mix(target):
        logits = lg[...]
        for e in range(experts):
            first = jnp.tanh(proj[:, e * rank:(e + 1) * rank]).astype(jnp.bfloat16)
            second = jnp.dot(first, cb[e], preferred_element_type=jnp.float32)
            total = jnp.sum(jnp.exp(logits - logits[:, e:e + 1]), axis=1, keepdims=True)
            gate = 1.0 / total
            target[:, e * rank:(e + 1) * rank] = (gate * jnp.tanh(second)).astype(jnp.bfloat16)

    def crossed(blend, maps, shift, c):
        return (
            jnp.dot(blend[...], maps[c], preferred_element_type=jnp.float32)
            + shift[:, columns(c)]
        )

    def relay(wait_chunk):
        line_event(0)
        clear()
        marks = [0] + [chunks * (d + 1) // layers - chunks // (2 * layers) for d in range(layers - 1)]
        marks += [chunks]

        def body(c):
            wait_chunk(c)
            gather_in(in1[c], c)

        for d in range(layers):
            if d == 1 or d > 1 and d < layers - 1:
                line_event(d)
            if 1 <= d < layers - 1:
                side_event(d - 1)
            each(body, marks[d], marks[d + 1])
        mix(sent)
        blend_over.start()
        if layers > 1:
            line_event(layers - 1)
        for d in range(max(layers - 2, 0), layers):
            side_event(d)

    def take_share(c):
        @pl.when(c % 2 != core)
        def _():
            await_share(c)

    @pl.when(me == 0)
    def _():
        load_g.wait()
        clear()

        def first(c):
            load_x(c).wait()
            load_v(c).wait()
            gather_in(xb[c], c)
        each(first)
        load_c.wait()
        load_b.wait()
        mix(bl)

        def own(c):
            load_u(c).wait()
            base = xb[c].astype(jnp.float32)
            out1[c] = (base + base * crossed(bl, ub, bb, c)).astype(jnp.bfloat16)
            put(out1.at[c], c).start()
        each(own)
        relay(lambda c: put(out1.at[c], c).wait_recv())
        bias_over.wait_recv()
        blend_over.wait_recv()

        def finish(c):
            take_share(c)
            ob[c] = (
                out1[c].astype(jnp.float32)
                + xb[c].astype(jnp.float32) * crossed(got, gu, b2, c)
            ).astype(jnp.bfloat16)
            put_out(c).start()
        each(finish)

    @pl.when(me == 1)
    def _():
        def send_x(c):
            return put(x_hbm.at[:, columns(c)], c)

        each(lambda c: send_x(c).start())
        load_g.wait()
        load_c.wait()
        load_b.wait()

        def ready(c):
            load_x(c).wait()
            load_v(c).wait()
            load_u(c).wait()
        each(ready)
        relay(lambda c: send_x(c).wait_recv())
        bias_over.wait_recv()
        blend_over.wait_recv()
        clear()

        def advance(c):
            take_share(c)
            base = xb[c].astype(jnp.float32)
            after = (base + base * crossed(got, gu, b2, c)).astype(jnp.bfloat16)
            out1[c] = after
            gather_in(after, c)
        each(advance)
        mix(bl)

        def finish(c):
            ob[c] = (
                out1[c].astype(jnp.float32)
                + xb[c].astype(jnp.float32) * crossed(bl, ub, bb, c)
            ).astype(jnp.bfloat16)
            put_out(c).start()
        each(finish)

    def drain(c):
        put(out1.at[c], c).wait_send()
        put_out(c).wait()
    each(drain)
    share_over.wait_send()
    bias_over.wait_send()
    blend_over.wait_send()
    for d in range(layers):
        line_event(d, True)
        side_event(d, True)


def pair_device(features, in_proj, mix_proj, out_proj, gate_proj, cross_bias):
    rows, depth = features.shape[2:]
    experts, rank = mix_proj.shape[1:3]
    inner = experts * rank
    chunks = lax.axis_size("dp")
    width = depth // chunks
    kind = jnp.bfloat16
    block = pltpu.VMEM((chunks, rows, width), kind)
    blend = pltpu.VMEM((rows, inner), kind)
    sems = pltpu.SemaphoreType.DMA((chunks,))
    two = pltpu.SemaphoreType.DMA((2,))
    anywhere = pl.BlockSpec(memory_space=pl.ANY)
    out = pl.pallas_call(
        relay_kernel,
        out_shape=jax.ShapeDtypeStruct((rows, depth), kind),
        in_specs=[anywhere] * 6,
        out_specs=anywhere,
        scratch_shapes=[
            block,
            pltpu.VMEM((chunks, width, inner), kind),
            pltpu.VMEM((experts, rank, rank), kind),
            pltpu.VMEM((chunks, inner, width), kind),
            pltpu.VMEM((experts, depth), kind),
            pltpu.VMEM((1, depth), jnp.float32),
            block, block, block,
            pltpu.VMEM((chunks, inner, width), kind),
            pltpu.VMEM((1, depth), jnp.float32),
            pltpu.VMEM((rows, inner), jnp.float32),
            pltpu.VMEM((rows, experts), jnp.float32),
            blend, blend, blend,
            sems, sems, sems, pltpu.SemaphoreType.DMA((3,)),
            sems, sems, sems,
            two, sems, sems, sems, sems, sems, two, two,
        ],
        compiler_params=pltpu.CompilerParams(
            collective_id=0, has_side_effects=True, vmem_limit_bytes=60 * 1024 * 1024
        ),
    )(features[0, 0], in_proj[0], mix_proj[0], out_proj[0], gate_proj[0], cross_bias)
    return out.reshape(features.shape)


def from_behind(block, axis, distance):
    devices = range(lax.axis_size(axis))
    route = [(i - distance, i) for i in devices if i - distance in devices]
    return lax.ppermute(block, axis, route)


def cross_layer(current, anchor, v_mat, c_mat, u_mat, gate_mat, shift_row):
    row_count = current.shape[0]
    expert_count = c_mat.shape[0]
    rank_size = c_mat.shape[1]
    projected = jnp.dot(current, v_mat, preferred_element_type=jnp.float32)
    inner_first = (
        jnp.tanh(projected).astype(jnp.bfloat16).reshape(row_count, expert_count, rank_size)
    )
    inner_second = jnp.einsum(
        "rek,ekj->rej", inner_first, c_mat, preferred_element_type=jnp.float32
    )
    logits = lax.dot_general(
        current, gate_mat, (((1,), (1,)), ((), ())), preferred_element_type=jnp.float32
    )
    gate_values = 1.0 / jnp.sum(jnp.exp(logits[:, None, :] - logits[:, :, None]), axis=2)
    blended = (gate_values[:, :, None] * jnp.tanh(inner_second)).astype(jnp.bfloat16)
    blended = blended.reshape(row_count, expert_count * rank_size)
    crossed = jnp.dot(blended, u_mat, preferred_element_type=jnp.float32)
    updated = current.astype(jnp.float32) + anchor.astype(jnp.float32) * (crossed + shift_row)
    return updated.astype(jnp.bfloat16)


def per_device(features, in_proj, mix_proj, out_proj, gate_proj, cross_bias):
    section_count = lax.axis_size("section")
    position = lax.axis_index("section")
    pieces = 1
    local_micro = features.shape[0]
    row_count = features.shape[2]
    feature_count = features.shape[3]
    piece_rows = row_count // pieces
    everyone = lax.all_gather(features, "section", axis=1, tiled=True)
    all_units = everyone.reshape(local_micro * section_count * pieces, piece_rows, feature_count)
    unit_count = all_units.shape[0]
    step_count = unit_count + section_count - 1
    v_mat = in_proj[0]
    c_mat = mix_proj[0]
    u_mat = out_proj[0]
    gate_mat = gate_proj[0]
    shift_row = cross_bias[0]

    def apply_layer(current, anchor):
        return cross_layer(current, anchor, v_mat, c_mat, u_mat, gate_mat, shift_row)

    def keep_input(current, anchor):
        return current

    def advance(carried, moment):
        incoming, outgoing, collected = carried
        unit_here = moment - position
        active = (unit_here >= 0) & (unit_here < unit_count)
        anchor = lax.dynamic_index_in_dim(
            all_units, jnp.clip(unit_here, 0, unit_count - 1), 0, keepdims=False
        )
        current = jnp.where(position == 0, anchor, incoming)
        result = lax.cond(active, apply_layer, keep_input, current, anchor)
        outgoing = jnp.where(position == section_count - 1, result, outgoing)
        held_unit = moment + position - 2 * section_count + 2
        arrived = (
            (held_unit >= 0)
            & (held_unit < unit_count)
            & (held_unit // pieces % section_count == position)
        )
        held_safe = jnp.clip(held_unit, 0, unit_count - 1)
        slot_index = held_safe // pieces // section_count * pieces + held_safe % pieces
        previous = lax.dynamic_index_in_dim(collected, slot_index, 0, keepdims=False)
        collected = lax.dynamic_update_index_in_dim(
            collected, jnp.where(arrived, outgoing, previous), slot_index, 0
        )
        return (result, outgoing, collected)

    def forward_step(carried, moment):
        result, outgoing, collected = advance(carried, moment)
        incoming = from_behind(result, "section", 1)
        return ((incoming, outgoing, collected), None)

    def cycle_step(carried, moment):
        moved, _ = forward_step(carried, moment)
        incoming, outgoing, collected = moved
        outgoing = from_behind(outgoing, "section", -1)
        return ((incoming, outgoing, collected), None)

    blank = jnp.zeros((piece_rows, feature_count), jnp.bfloat16)
    holding = jnp.zeros((local_micro * pieces, piece_rows, feature_count), jnp.bfloat16)
    carried, _ = lax.scan(
        forward_step, (blank, blank, holding), jnp.arange(0, section_count - 1, dtype=jnp.int32)
    )
    carried, _ = lax.scan(
        cycle_step, carried, jnp.arange(section_count - 1, step_count - 1, dtype=jnp.int32)
    )
    _, _, collected = advance(carried, jnp.int32(step_count - 1))
    return collected.reshape(local_micro, 1, row_count, feature_count)


def solution(mesh):
    placed = (
        P(None, "section", "dp", None),
        P("section", None, None),
        P("section", None, None, None),
        P("section", None, None),
        P("section", None, None),
        P("section", None),
    )
    sections, groups = mesh.shape["section"], mesh.shape["dp"]

    def choose(features, *weights):
        whole = sections == 2 and features.shape[0] == 1 and groups % GROUP == 0
        whole = whole and features.shape[3] % (groups * 128) == 0
        return (pair_device if whole else per_device)(features, *weights)

    return jax.shard_map(
        choose,
        mesh=mesh,
        in_specs=placed,
        out_specs=P(None, "section", "dp", None),
        check_vma=False,
    )
```

```python
import jax
import jax.numpy as jnp
from jax import lax
from jax.experimental import pallas as pl
from jax.experimental.pallas import tpu as pltpu
from jax.sharding import PartitionSpec as P

GROUP = 4
BATCH = 8
MESH = pl.DeviceIdType.MESH
LINE_AT = lambda d, chunks, layers: d * (d + 1) // 2 * chunks // 16 if d < layers - 1 else chunks - 2
SIDE_AT = lambda d, chunks, layers: (4 * d + 2) * chunks // 16 if d < layers - 2 else chunks - 2 if d < layers - 1 else chunks + 1


def relay_kernel(
    x_hbm, v_hbm, c_hbm, u_hbm, g_hbm, b_hbm, o_hbm,
    xb, vb, cb, ub, gb, bb, in1, out1, ob, gu, b2, proj, lg, bl, sent, got,
    lx, lv, lu, lw, s1, r1, so, sx, rg, s_up, s_down, s_side, s_core, s3, r3,
):
    chunks, rows, width = xb.shape
    experts, rank, _ = cb.shape
    layers = chunks // GROUP
    me = lax.axis_index("section")
    peer = 1 - me
    mine = lax.axis_index("dp")
    level = mine // GROUP
    core = mine % 2
    side = mine + 2 - 4 * (mine // 2 % 2)
    twin = mine + 1 - 2 * core

    def columns(c):
        return pl.ds(pl.multiple_of(c * width, width), width)

    def load_x(c):
        return pltpu.make_async_copy(x_hbm.at[:, columns(c)], xb.at[c], lx.at[c])

    def load_v(c):
        return pltpu.make_async_copy(v_hbm.at[columns(c)], vb.at[c], lv.at[c])

    def load_u(c):
        return pltpu.make_async_copy(u_hbm.at[:, columns(c)], ub.at[c], lu.at[c])

    load_c = pltpu.make_async_copy(c_hbm, cb, lw.at[0])
    load_g = pltpu.make_async_copy(g_hbm, gb, lw.at[1])
    load_b = pltpu.make_async_copy(b_hbm, bb, lw.at[2])

    def cross_over(src, dst, send, recv):
        return pltpu.make_async_remote_copy(
            src_ref=src, dst_ref=dst, send_sem=send, recv_sem=recv,
            device_id={"section": peer}, device_id_type=MESH,
        )

    def put(src, c):
        return cross_over(src, in1.at[c], s1.at[c], r1.at[c])

    def put_out(c):
        return pltpu.make_async_copy(ob.at[c], o_hbm.at[:, columns(c)], so.at[c])

    share_over = cross_over(u_hbm.at[:, columns(mine)], gu.at[mine], sx.at[0], rg.at[mine])
    bias_over = cross_over(b_hbm, b2, s3.at[0], r3.at[0])
    blend_over = cross_over(sent, got, s3.at[1], r3.at[1])

    def hand(share, target, send):
        return pltpu.make_async_remote_copy(
            src_ref=gu.at[share], dst_ref=gu.at[share], send_sem=send.at[share],
            recv_sem=rg.at[share], device_id={"dp": target}, device_id_type=MESH,
        )

    def await_share(share):
        hand(share, side, s_side).wait_recv()

    def pass_on(copy, finish):
        if finish:
            copy.wait_send()
        else:
            copy.start()

    def along(share, go_up, go_down, finish):
        if go_up:
            @pl.when(level < layers - 1)
            def _():
                pass_on(hand(share, mine + GROUP, s_up), finish)
        if go_down:
            @pl.when(level > 0)
            def _():
                pass_on(hand(share, mine - GROUP, s_down), finish)
        pass_on(hand(share, side, s_side), finish)
        pass_on(hand(share, twin, s_core), finish)

    def line_event(d, finish=False):
        def act(share, go_up, go_down):
            if not finish:
                await_share(share)
            along(share, go_up, go_down, finish)
        if d == 0:
            act(mine, True, True)
            return
        pl.when(level >= d)(lambda: act(mine - GROUP * d, True, False))
        pl.when(level + d < layers)(lambda: act(mine + GROUP * d, False, True))

    def side_event(d, finish=False):
        def act(share):
            if not finish:
                await_share(share)
            pass_on(hand(share, twin, s_core), finish)
        if d == 0:
            act(side)
            return
        pl.when(level >= d)(lambda: act(side - GROUP * d))
        pl.when(level + d < layers)(lambda: act(side + GROUP * d))

    def each(body, start=0, stop=chunks):
        def step(c, carry):
            body(c)
            return carry
        lax.fori_loop(start, stop, step, 0)

    def batches(body):
        def step(i, carry):
            body([i * BATCH + j for j in range(BATCH)])
            return carry
        lax.fori_loop(0, chunks // BATCH, step, 0)

    barrier = pltpu.get_barrier_semaphore()
    pl.semaphore_signal(barrier, inc=1, device_id={"section": peer}, device_id_type=MESH)
    pl.semaphore_signal(barrier, inc=1, device_id={"dp": side}, device_id_type=MESH)
    pl.semaphore_signal(barrier, inc=1, device_id={"dp": twin}, device_id_type=MESH)

    @pl.when(level < layers - 1)
    def _():
        pl.semaphore_signal(barrier, inc=1, device_id={"dp": mine + GROUP}, device_id_type=MESH)

    @pl.when(level > 0)
    def _():
        pl.semaphore_signal(barrier, inc=1, device_id={"dp": mine - GROUP}, device_id_type=MESH)

    load_g.start()

    def load_first(c):
        load_x(c).start()
        load_v(c).start()
    each(load_first)
    load_c.start()
    load_b.start()
    each(lambda c: load_u(c).start())
    inside = (level > 0) & (level < layers - 1)

    @pl.when(inside)
    def _():
        pl.semaphore_wait(barrier, 5)

    @pl.when(jnp.logical_not(inside))
    def _():
        pl.semaphore_wait(barrier, 4 if layers > 1 else 3)

    share_over.start()
    bias_over.start()

    def clear():
        proj[...] = jnp.zeros_like(proj)
        lg[...] = jnp.zeros_like(lg)

    def gather_in(parts, cs):
        both = (((1,), (1,)), ((), ()))
        proj[...] += sum(
            jnp.dot(part, vb[c], preferred_element_type=jnp.float32) for part, c in zip(parts, cs)
        )
        lg[...] += sum(
            lax.dot_general(part, gb[:, columns(c)], both, preferred_element_type=jnp.float32)
            for part, c in zip(parts, cs)
        )

    def mix(target):
        logits = lg[...]
        for e in range(experts):
            first = jnp.tanh(proj[:, e * rank:(e + 1) * rank]).astype(jnp.bfloat16)
            second = jnp.dot(first, cb[e], preferred_element_type=jnp.float32)
            total = jnp.sum(jnp.exp(logits - logits[:, e:e + 1]), axis=1, keepdims=True)
            gate = 1.0 / total
            target[:, e * rank:(e + 1) * rank] = (gate * jnp.tanh(second)).astype(jnp.bfloat16)

    def crossed(blend, maps, shift, c):
        return (
            jnp.dot(blend[...], maps[c], preferred_element_type=jnp.float32)
            + shift[:, columns(c)]
        )

    def relay(wait_chunk):
        plan = {}
        for d in range(layers):
            plan.setdefault(LINE_AT(d, chunks, layers), []).append((line_event, d))
            plan.setdefault(SIDE_AT(d, chunks, layers), []).append((side_event, d))
        clear()

        def body(c):
            wait_chunk(c)
            gather_in([in1[c]], [c])

        at = 0
        for mark in sorted(plan):
            if mark > chunks:
                break
            each(body, at, mark)
            at = mark
            for event, d in plan[mark]:
                event(d)
        each(body, at, chunks)
        mix(sent)
        blend_over.start()
        for mark in sorted(plan):
            if mark > chunks:
                for event, d in plan[mark]:
                    event(d)

    def take_share(c):
        @pl.when(c % 2 != core)
        def _():
            await_share(c)

    @pl.when(me == 0)
    def _():
        load_g.wait()
        clear()

        def first(cs):
            for c in cs:
                load_x(c).wait()
                load_v(c).wait()
            gather_in([xb[c] for c in cs], cs)
        batches(first)
        load_c.wait()
        load_b.wait()
        mix(bl)

        def own(c):
            load_u(c).wait()
            base = xb[c].astype(jnp.float32)
            out1[c] = (base + base * crossed(bl, ub, bb, c)).astype(jnp.bfloat16)
            put(out1.at[c], c).start()
        each(own)
        relay(lambda c: put(out1.at[c], c).wait_recv())
        bias_over.wait_recv()
        blend_over.wait_recv()

        each(take_share)

        def finish(cs):
            for c in cs:
                ob[c] = (
                    out1[c].astype(jnp.float32)
                    + xb[c].astype(jnp.float32) * crossed(got, gu, b2, c)
                ).astype(jnp.bfloat16)
            for c in cs:
                put_out(c).start()
        batches(finish)

    @pl.when(me == 1)
    def _():
        def send_x(c):
            return put(x_hbm.at[:, columns(c)], c)

        each(lambda c: send_x(c).start())
        load_g.wait()
        load_c.wait()
        load_b.wait()

        def ready(c):
            load_x(c).wait()
            load_v(c).wait()
            load_u(c).wait()
        each(ready)
        relay(lambda c: send_x(c).wait_recv())
        bias_over.wait_recv()
        blend_over.wait_recv()
        clear()

        each(take_share)

        def advance(cs):
            parts = []
            for c in cs:
                base = xb[c].astype(jnp.float32)
                parts.append((base + base * crossed(got, gu, b2, c)).astype(jnp.bfloat16))
            for c, part in zip(cs, parts):
                out1[c] = part
            gather_in(parts, cs)
        batches(advance)
        mix(bl)

        def finish(cs):
            for c in cs:
                ob[c] = (
                    out1[c].astype(jnp.float32)
                    + xb[c].astype(jnp.float32) * crossed(bl, ub, bb, c)
                ).astype(jnp.bfloat16)
            for c in cs:
                put_out(c).start()
        batches(finish)

    def drain(c):
        put(out1.at[c], c).wait_send()
        put_out(c).wait()
    each(drain)
    share_over.wait_send()
    bias_over.wait_send()
    blend_over.wait_send()
    for d in range(layers):
        line_event(d, True)
        side_event(d, True)


def pair_device(features, in_proj, mix_proj, out_proj, gate_proj, cross_bias):
    rows, depth = features.shape[2:]
    experts, rank = mix_proj.shape[1:3]
    inner = experts * rank
    chunks = lax.axis_size("dp")
    width = depth // chunks
    kind = jnp.bfloat16
    block = pltpu.VMEM((chunks, rows, width), kind)
    blend = pltpu.VMEM((rows, inner), kind)
    sems = pltpu.SemaphoreType.DMA((chunks,))
    two = pltpu.SemaphoreType.DMA((2,))
    anywhere = pl.BlockSpec(memory_space=pl.ANY)
    out = pl.pallas_call(
        relay_kernel,
        out_shape=jax.ShapeDtypeStruct((rows, depth), kind),
        in_specs=[anywhere] * 6,
        out_specs=anywhere,
        scratch_shapes=[
            block,
            pltpu.VMEM((chunks, width, inner), kind),
            pltpu.VMEM((experts, rank, rank), kind),
            pltpu.VMEM((chunks, inner, width), kind),
            pltpu.VMEM((experts, depth), kind),
            pltpu.VMEM((1, depth), jnp.float32),
            block, block, block,
            pltpu.VMEM((chunks, inner, width), kind),
            pltpu.VMEM((1, depth), jnp.float32),
            pltpu.VMEM((rows, inner), jnp.float32),
            pltpu.VMEM((rows, experts), jnp.float32),
            blend, blend, blend,
            sems, sems, sems, pltpu.SemaphoreType.DMA((3,)),
            sems, sems, sems,
            two, sems, sems, sems, sems, sems, two, two,
        ],
        compiler_params=pltpu.CompilerParams(
            collective_id=0, has_side_effects=True, vmem_limit_bytes=60 * 1024 * 1024
        ),
    )(features[0, 0], in_proj[0], mix_proj[0], out_proj[0], gate_proj[0], cross_bias)
    return out.reshape(features.shape)


def from_behind(block, axis, distance):
    devices = range(lax.axis_size(axis))
    route = [(i - distance, i) for i in devices if i - distance in devices]
    return lax.ppermute(block, axis, route)


def cross_layer(current, anchor, v_mat, c_mat, u_mat, gate_mat, shift_row):
    row_count = current.shape[0]
    expert_count = c_mat.shape[0]
    rank_size = c_mat.shape[1]
    projected = jnp.dot(current, v_mat, preferred_element_type=jnp.float32)
    inner_first = (
        jnp.tanh(projected).astype(jnp.bfloat16).reshape(row_count, expert_count, rank_size)
    )
    inner_second = jnp.einsum(
        "rek,ekj->rej", inner_first, c_mat, preferred_element_type=jnp.float32
    )
    logits = lax.dot_general(
        current, gate_mat, (((1,), (1,)), ((), ())), preferred_element_type=jnp.float32
    )
    gate_values = 1.0 / jnp.sum(jnp.exp(logits[:, None, :] - logits[:, :, None]), axis=2)
    blended = (gate_values[:, :, None] * jnp.tanh(inner_second)).astype(jnp.bfloat16)
    blended = blended.reshape(row_count, expert_count * rank_size)
    crossed = jnp.dot(blended, u_mat, preferred_element_type=jnp.float32)
    updated = current.astype(jnp.float32) + anchor.astype(jnp.float32) * (crossed + shift_row)
    return updated.astype(jnp.bfloat16)


def per_device(features, in_proj, mix_proj, out_proj, gate_proj, cross_bias):
    section_count = lax.axis_size("section")
    position = lax.axis_index("section")
    pieces = 1
    local_micro = features.shape[0]
    row_count = features.shape[2]
    feature_count = features.shape[3]
    piece_rows = row_count // pieces
    everyone = lax.all_gather(features, "section", axis=1, tiled=True)
    all_units = everyone.reshape(local_micro * section_count * pieces, piece_rows, feature_count)
    unit_count = all_units.shape[0]
    step_count = unit_count + section_count - 1
    v_mat = in_proj[0]
    c_mat = mix_proj[0]
    u_mat = out_proj[0]
    gate_mat = gate_proj[0]
    shift_row = cross_bias[0]

    def apply_layer(current, anchor):
        return cross_layer(current, anchor, v_mat, c_mat, u_mat, gate_mat, shift_row)

    def keep_input(current, anchor):
        return current

    def advance(carried, moment):
        incoming, outgoing, collected = carried
        unit_here = moment - position
        active = (unit_here >= 0) & (unit_here < unit_count)
        anchor = lax.dynamic_index_in_dim(
            all_units, jnp.clip(unit_here, 0, unit_count - 1), 0, keepdims=False
        )
        current = jnp.where(position == 0, anchor, incoming)
        result = lax.cond(active, apply_layer, keep_input, current, anchor)
        outgoing = jnp.where(position == section_count - 1, result, outgoing)
        held_unit = moment + position - 2 * section_count + 2
        arrived = (
            (held_unit >= 0)
            & (held_unit < unit_count)
            & (held_unit // pieces % section_count == position)
        )
        held_safe = jnp.clip(held_unit, 0, unit_count - 1)
        slot_index = held_safe // pieces // section_count * pieces + held_safe % pieces
        previous = lax.dynamic_index_in_dim(collected, slot_index, 0, keepdims=False)
        collected = lax.dynamic_update_index_in_dim(
            collected, jnp.where(arrived, outgoing, previous), slot_index, 0
        )
        return (result, outgoing, collected)

    def forward_step(carried, moment):
        result, outgoing, collected = advance(carried, moment)
        incoming = from_behind(result, "section", 1)
        return ((incoming, outgoing, collected), None)

    def cycle_step(carried, moment):
        moved, _ = forward_step(carried, moment)
        incoming, outgoing, collected = moved
        outgoing = from_behind(outgoing, "section", -1)
        return ((incoming, outgoing, collected), None)

    blank = jnp.zeros((piece_rows, feature_count), jnp.bfloat16)
    holding = jnp.zeros((local_micro * pieces, piece_rows, feature_count), jnp.bfloat16)
    carried, _ = lax.scan(
        forward_step, (blank, blank, holding), jnp.arange(0, section_count - 1, dtype=jnp.int32)
    )
    carried, _ = lax.scan(
        cycle_step, carried, jnp.arange(section_count - 1, step_count - 1, dtype=jnp.int32)
    )
    _, _, collected = advance(carried, jnp.int32(step_count - 1))
    return collected.reshape(local_micro, 1, row_count, feature_count)


def solution(mesh):
    placed = (
        P(None, "section", "dp", None),
        P("section", None, None),
        P("section", None, None, None),
        P("section", None, None),
        P("section", None, None),
        P("section", None),
    )
    sections, groups = mesh.shape["section"], mesh.shape["dp"]

    def choose(features, *weights):
        whole = sections == 2 and features.shape[0] == 1 and groups % BATCH == 0
        whole = whole and features.shape[3] % (groups * 128) == 0
        return (pair_device if whole else per_device)(features, *weights)

    return jax.shard_map(
        choose,
        mesh=mesh,
        in_specs=placed,
        out_specs=P(None, "section", "dp", None),
        check_vma=False,
    )
```

```python
import jax
import jax.numpy as jnp
from jax import lax
from jax.experimental import pallas as pl
from jax.experimental.pallas import tpu as pltpu
from jax.sharding import PartitionSpec as P

GROUP = 4
BATCH = 8
MESH = pl.DeviceIdType.MESH
LINE_AT = lambda d, chunks, layers: d * (d + 1) // 2 * chunks // 16 if d < layers - 1 else chunks - 2
SIDE_AT = lambda d, chunks, layers: (4 * d + 2) * chunks // 16 if d < layers - 2 else chunks - 2 if d < layers - 1 else chunks + 1


def relay_kernel(
    x_hbm, v_hbm, c_hbm, u_hbm, g_hbm, b_hbm, o_hbm,
    xb, vb, cb, ub, gb, bb, in1, out1, ob, gu, b2, proj, lg, bl, sent, got,
    lx, lv, lu, lw, s1, r1, so, sx, rg, s_up, s_down, s_side, s_core, s3, r3,
):
    chunks, rows, width = xb.shape
    experts, rank, _ = cb.shape
    layers = chunks // GROUP
    me = lax.axis_index("section")
    peer = 1 - me
    mine = lax.axis_index("dp")
    level = mine // GROUP
    core = mine % 2
    side = mine + 2 - 4 * (mine // 2 % 2)
    twin = mine + 1 - 2 * core

    def columns(c):
        return pl.ds(pl.multiple_of(c * width, width), width)

    def load_x(c):
        return pltpu.make_async_copy(x_hbm.at[:, columns(c)], xb.at[c], lx.at[c])

    def load_v(c):
        return pltpu.make_async_copy(v_hbm.at[columns(c)], vb.at[c], lv.at[c])

    def load_u(c):
        return pltpu.make_async_copy(u_hbm.at[:, columns(c)], ub.at[c], lu.at[c])

    load_c = pltpu.make_async_copy(c_hbm, cb, lw.at[0])
    load_g = pltpu.make_async_copy(g_hbm, gb, lw.at[1])
    load_b = pltpu.make_async_copy(b_hbm, bb, lw.at[2])

    def cross_over(src, dst, send, recv):
        return pltpu.make_async_remote_copy(
            src_ref=src, dst_ref=dst, send_sem=send, recv_sem=recv,
            device_id={"section": peer}, device_id_type=MESH,
        )

    def put(src, c):
        return cross_over(src, in1.at[c], s1.at[c], r1.at[c])

    def put_out(c):
        return pltpu.make_async_copy(ob.at[c], o_hbm.at[:, columns(c)], so.at[c])

    share_over = cross_over(u_hbm.at[:, columns(mine)], gu.at[mine], sx.at[0], rg.at[mine])
    bias_over = cross_over(b_hbm, b2, s3.at[0], r3.at[0])

    def blend_over(e):
        part = (slice(None), pl.ds(e * rank, rank))
        return cross_over(sent.at[part], got.at[part], s3.at[1 + e], r3.at[1 + e])

    def hand(share, target, send):
        return pltpu.make_async_remote_copy(
            src_ref=gu.at[share], dst_ref=gu.at[share], send_sem=send.at[share],
            recv_sem=rg.at[share], device_id={"dp": target}, device_id_type=MESH,
        )

    def await_share(share):
        hand(share, side, s_side).wait_recv()

    def pass_on(copy, finish):
        if finish:
            copy.wait_send()
        else:
            copy.start()

    def along(share, go_up, go_down, finish):
        if go_up:
            @pl.when(level < layers - 1)
            def _():
                pass_on(hand(share, mine + GROUP, s_up), finish)
        if go_down:
            @pl.when(level > 0)
            def _():
                pass_on(hand(share, mine - GROUP, s_down), finish)
        pass_on(hand(share, side, s_side), finish)
        pass_on(hand(share, twin, s_core), finish)

    def line_event(d, finish=False):
        def act(share, go_up, go_down):
            if not finish:
                await_share(share)
            along(share, go_up, go_down, finish)
        if d == 0:
            act(mine, True, True)
            return
        pl.when(level >= d)(lambda: act(mine - GROUP * d, True, False))
        pl.when(level + d < layers)(lambda: act(mine + GROUP * d, False, True))

    def side_event(d, finish=False):
        def act(share):
            if not finish:
                await_share(share)
            pass_on(hand(share, twin, s_core), finish)
        if d == 0:
            act(side)
            return
        pl.when(level >= d)(lambda: act(side - GROUP * d))
        pl.when(level + d < layers)(lambda: act(side + GROUP * d))

    def each(body, start=0, stop=chunks):
        def step(c, carry):
            body(c)
            return carry
        lax.fori_loop(start, stop, step, 0)

    def batches(body):
        def step(i, carry):
            body([i * BATCH + j for j in range(BATCH)])
            return carry
        lax.fori_loop(0, chunks // BATCH, step, 0)

    barrier = pltpu.get_barrier_semaphore()
    pl.semaphore_signal(barrier, inc=1, device_id={"section": peer}, device_id_type=MESH)
    pl.semaphore_signal(barrier, inc=1, device_id={"dp": side}, device_id_type=MESH)
    pl.semaphore_signal(barrier, inc=1, device_id={"dp": twin}, device_id_type=MESH)

    @pl.when(level < layers - 1)
    def _():
        pl.semaphore_signal(barrier, inc=1, device_id={"dp": mine + GROUP}, device_id_type=MESH)

    @pl.when(level > 0)
    def _():
        pl.semaphore_signal(barrier, inc=1, device_id={"dp": mine - GROUP}, device_id_type=MESH)

    load_g.start()

    def load_first(c):
        load_x(c).start()
        load_v(c).start()
    each(load_first)
    load_c.start()
    load_b.start()
    each(lambda c: load_u(c).start())
    inside = (level > 0) & (level < layers - 1)

    @pl.when(inside)
    def _():
        pl.semaphore_wait(barrier, 5)

    @pl.when(jnp.logical_not(inside))
    def _():
        pl.semaphore_wait(barrier, 4 if layers > 1 else 3)

    share_over.start()
    bias_over.start()

    def clear():
        proj[...] = jnp.zeros_like(proj)
        lg[...] = jnp.zeros_like(lg)

    def gather_in(parts, cs):
        both = (((1,), (1,)), ((), ()))
        proj[...] += sum(
            jnp.dot(part, vb[c], preferred_element_type=jnp.float32) for part, c in zip(parts, cs)
        )
        lg[...] += sum(
            lax.dot_general(part, gb[:, columns(c)], both, preferred_element_type=jnp.float32)
            for part, c in zip(parts, cs)
        )

    def mix(target, after=None):
        logits = lg[...]
        for e in range(experts):
            first = jnp.tanh(proj[:, e * rank:(e + 1) * rank]).astype(jnp.bfloat16)
            second = jnp.dot(first, cb[e], preferred_element_type=jnp.float32)
            total = jnp.sum(jnp.exp(logits - logits[:, e:e + 1]), axis=1, keepdims=True)
            gate = 1.0 / total
            target[:, e * rank:(e + 1) * rank] = (gate * jnp.tanh(second)).astype(jnp.bfloat16)
            if after is not None:
                after(e)

    def crossed(blend, maps, shift, c):
        return (
            jnp.dot(blend[...], maps[c], preferred_element_type=jnp.float32)
            + shift[:, columns(c)]
        )

    def relay(wait_chunk):
        plan = {}
        for d in range(layers):
            plan.setdefault(LINE_AT(d, chunks, layers), []).append((line_event, d))
            plan.setdefault(SIDE_AT(d, chunks, layers), []).append((side_event, d))
        clear()

        def body(c):
            wait_chunk(c)
            gather_in([in1[c]], [c])

        at = 0
        for mark in sorted(plan):
            if mark > chunks:
                break
            each(body, at, mark)
            at = mark
            for event, d in plan[mark]:
                event(d)
        each(body, at, chunks)
        mix(sent, lambda e: blend_over(e).start())
        for mark in sorted(plan):
            if mark > chunks:
                for event, d in plan[mark]:
                    event(d)

    def take_share(c):
        @pl.when(c % 2 != core)
        def _():
            await_share(c)

    @pl.when(me == 0)
    def _():
        load_g.wait()
        clear()

        def first(cs):
            for c in cs:
                load_x(c).wait()
                load_v(c).wait()
            gather_in([xb[c] for c in cs], cs)
        batches(first)
        load_c.wait()
        load_b.wait()
        mix(bl)

        def own(c):
            load_u(c).wait()
            base = xb[c].astype(jnp.float32)
            out1[c] = (base + base * crossed(bl, ub, bb, c)).astype(jnp.bfloat16)
            put(out1.at[c], c).start()
        each(own)
        relay(lambda c: put(out1.at[c], c).wait_recv())
        bias_over.wait_recv()
        for e in range(experts):
            blend_over(e).wait_recv()

        each(take_share)

        def finish(cs):
            for c in cs:
                ob[c] = (
                    out1[c].astype(jnp.float32)
                    + xb[c].astype(jnp.float32) * crossed(got, gu, b2, c)
                ).astype(jnp.bfloat16)
            for c in cs:
                put_out(c).start()
        batches(finish)

    @pl.when(me == 1)
    def _():
        def send_x(c):
            return put(x_hbm.at[:, columns(c)], c)

        each(lambda c: send_x(c).start())
        load_g.wait()
        load_c.wait()
        load_b.wait()

        def ready(c):
            load_x(c).wait()
            load_v(c).wait()
            load_u(c).wait()
        each(ready)
        relay(lambda c: send_x(c).wait_recv())
        bias_over.wait_recv()
        for e in range(experts):
            blend_over(e).wait_recv()
        clear()

        each(take_share)

        def advance(cs):
            parts = []
            for c in cs:
                base = xb[c].astype(jnp.float32)
                parts.append((base + base * crossed(got, gu, b2, c)).astype(jnp.bfloat16))
            for c, part in zip(cs, parts):
                out1[c] = part
            gather_in(parts, cs)
        batches(advance)
        mix(bl)

        def finish(cs):
            for c in cs:
                ob[c] = (
                    out1[c].astype(jnp.float32)
                    + xb[c].astype(jnp.float32) * crossed(bl, ub, bb, c)
                ).astype(jnp.bfloat16)
            for c in cs:
                put_out(c).start()
        batches(finish)

    def drain(c):
        put(out1.at[c], c).wait_send()
        put_out(c).wait()
    each(drain)
    share_over.wait_send()
    bias_over.wait_send()
    for e in range(experts):
        blend_over(e).wait_send()
    for d in range(layers):
        line_event(d, True)
        side_event(d, True)


def pair_device(features, in_proj, mix_proj, out_proj, gate_proj, cross_bias):
    rows, depth = features.shape[2:]
    experts, rank = mix_proj.shape[1:3]
    inner = experts * rank
    chunks = lax.axis_size("dp")
    width = depth // chunks
    kind = jnp.bfloat16
    block = pltpu.VMEM((chunks, rows, width), kind)
    blend = pltpu.VMEM((rows, inner), kind)
    sems = pltpu.SemaphoreType.DMA((chunks,))
    two = pltpu.SemaphoreType.DMA((2,))
    extra = pltpu.SemaphoreType.DMA((1 + experts,))
    anywhere = pl.BlockSpec(memory_space=pl.ANY)
    out = pl.pallas_call(
        relay_kernel,
        out_shape=jax.ShapeDtypeStruct((rows, depth), kind),
        in_specs=[anywhere] * 6,
        out_specs=anywhere,
        scratch_shapes=[
            block,
            pltpu.VMEM((chunks, width, inner), kind),
            pltpu.VMEM((experts, rank, rank), kind),
            pltpu.VMEM((chunks, inner, width), kind),
            pltpu.VMEM((experts, depth), kind),
            pltpu.VMEM((1, depth), jnp.float32),
            block, block, block,
            pltpu.VMEM((chunks, inner, width), kind),
            pltpu.VMEM((1, depth), jnp.float32),
            pltpu.VMEM((rows, inner), jnp.float32),
            pltpu.VMEM((rows, experts), jnp.float32),
            blend, blend, blend,
            sems, sems, sems, pltpu.SemaphoreType.DMA((3,)),
            sems, sems, sems,
            two, sems, sems, sems, sems, sems, extra, extra,
        ],
        compiler_params=pltpu.CompilerParams(
            collective_id=0, has_side_effects=True, vmem_limit_bytes=60 * 1024 * 1024
        ),
    )(features[0, 0], in_proj[0], mix_proj[0], out_proj[0], gate_proj[0], cross_bias)
    return out.reshape(features.shape)


def from_behind(block, axis, distance):
    devices = range(lax.axis_size(axis))
    route = [(i - distance, i) for i in devices if i - distance in devices]
    return lax.ppermute(block, axis, route)


def cross_layer(current, anchor, v_mat, c_mat, u_mat, gate_mat, shift_row):
    row_count = current.shape[0]
    expert_count = c_mat.shape[0]
    rank_size = c_mat.shape[1]
    projected = jnp.dot(current, v_mat, preferred_element_type=jnp.float32)
    inner_first = (
        jnp.tanh(projected).astype(jnp.bfloat16).reshape(row_count, expert_count, rank_size)
    )
    inner_second = jnp.einsum(
        "rek,ekj->rej", inner_first, c_mat, preferred_element_type=jnp.float32
    )
    logits = lax.dot_general(
        current, gate_mat, (((1,), (1,)), ((), ())), preferred_element_type=jnp.float32
    )
    gate_values = 1.0 / jnp.sum(jnp.exp(logits[:, None, :] - logits[:, :, None]), axis=2)
    blended = (gate_values[:, :, None] * jnp.tanh(inner_second)).astype(jnp.bfloat16)
    blended = blended.reshape(row_count, expert_count * rank_size)
    crossed = jnp.dot(blended, u_mat, preferred_element_type=jnp.float32)
    updated = current.astype(jnp.float32) + anchor.astype(jnp.float32) * (crossed + shift_row)
    return updated.astype(jnp.bfloat16)


def per_device(features, in_proj, mix_proj, out_proj, gate_proj, cross_bias):
    section_count = lax.axis_size("section")
    position = lax.axis_index("section")
    pieces = 1
    local_micro = features.shape[0]
    row_count = features.shape[2]
    feature_count = features.shape[3]
    piece_rows = row_count // pieces
    everyone = lax.all_gather(features, "section", axis=1, tiled=True)
    all_units = everyone.reshape(local_micro * section_count * pieces, piece_rows, feature_count)
    unit_count = all_units.shape[0]
    step_count = unit_count + section_count - 1
    v_mat = in_proj[0]
    c_mat = mix_proj[0]
    u_mat = out_proj[0]
    gate_mat = gate_proj[0]
    shift_row = cross_bias[0]

    def apply_layer(current, anchor):
        return cross_layer(current, anchor, v_mat, c_mat, u_mat, gate_mat, shift_row)

    def keep_input(current, anchor):
        return current

    def advance(carried, moment):
        incoming, outgoing, collected = carried
        unit_here = moment - position
        active = (unit_here >= 0) & (unit_here < unit_count)
        anchor = lax.dynamic_index_in_dim(
            all_units, jnp.clip(unit_here, 0, unit_count - 1), 0, keepdims=False
        )
        current = jnp.where(position == 0, anchor, incoming)
        result = lax.cond(active, apply_layer, keep_input, current, anchor)
        outgoing = jnp.where(position == section_count - 1, result, outgoing)
        held_unit = moment + position - 2 * section_count + 2
        arrived = (
            (held_unit >= 0)
            & (held_unit < unit_count)
            & (held_unit // pieces % section_count == position)
        )
        held_safe = jnp.clip(held_unit, 0, unit_count - 1)
        slot_index = held_safe // pieces // section_count * pieces + held_safe % pieces
        previous = lax.dynamic_index_in_dim(collected, slot_index, 0, keepdims=False)
        collected = lax.dynamic_update_index_in_dim(
            collected, jnp.where(arrived, outgoing, previous), slot_index, 0
        )
        return (result, outgoing, collected)

    def forward_step(carried, moment):
        result, outgoing, collected = advance(carried, moment)
        incoming = from_behind(result, "section", 1)
        return ((incoming, outgoing, collected), None)

    def cycle_step(carried, moment):
        moved, _ = forward_step(carried, moment)
        incoming, outgoing, collected = moved
        outgoing = from_behind(outgoing, "section", -1)
        return ((incoming, outgoing, collected), None)

    blank = jnp.zeros((piece_rows, feature_count), jnp.bfloat16)
    holding = jnp.zeros((local_micro * pieces, piece_rows, feature_count), jnp.bfloat16)
    carried, _ = lax.scan(
        forward_step, (blank, blank, holding), jnp.arange(0, section_count - 1, dtype=jnp.int32)
    )
    carried, _ = lax.scan(
        cycle_step, carried, jnp.arange(section_count - 1, step_count - 1, dtype=jnp.int32)
    )
    _, _, collected = advance(carried, jnp.int32(step_count - 1))
    return collected.reshape(local_micro, 1, row_count, feature_count)


def solution(mesh):
    placed = (
        P(None, "section", "dp", None),
        P("section", None, None),
        P("section", None, None, None),
        P("section", None, None),
        P("section", None, None),
        P("section", None),
    )
    sections, groups = mesh.shape["section"], mesh.shape["dp"]

    def choose(features, *weights):
        whole = sections == 2 and features.shape[0] == 1 and groups % BATCH == 0
        whole = whole and features.shape[3] % (groups * 128) == 0
        return (pair_device if whole else per_device)(features, *weights)

    return jax.shard_map(
        choose,
        mesh=mesh,
        in_specs=placed,
        out_specs=P(None, "section", "dp", None),
        check_vma=False,
    )
```
